16 devices in a mesh: dp: 2 (over y, z), tp: 8 (over x, core).
Axes of the slice: x: 4, y: 2, z: 1, core: 2. Of those that a mesh axis runs over, the one named last changes fastest.
The devices are a block of a 4x4x8 slice.
Arguments:
- x_in: bfloat16 [512, 2048], P('dp'), parts along dimension 0
- lengths: int32 [512], P('dp'), parts along dimension 0
- k_cache: bfloat16 [2, 512, 256, 8, 128], P(None, 'dp', None, 'tp'), parts along dimension 1
- v_cache: bfloat16 [2, 512, 256, 8, 128], P(None, 'dp', None, 'tp'), parts along dimension 1
- g_attn: bfloat16 [2, 2048], replicated
- w_q: bfloat16 [2, 2048, 2048], P(None, None, 'tp')
- b_q: bfloat16 [2, 2048], P(None, 'tp')
- w_k: bfloat16 [2, 2048, 1024], P(None, None, 'tp')
- b_k: bfloat16 [2, 1024], P(None, 'tp')
- w_v: bfloat16 [2, 2048, 1024], P(None, None, 'tp')
- b_v: bfloat16 [2, 1024], P(None, 'tp')
- w_o: bfloat16 [2, 2048, 2048], P(None, 'tp')
- g_mlp: bfloat16 [2, 2048], replicated
- w_gate: bfloat16 [2, 2048, 11008], P(None, None, 'tp')
- w_up: bfloat16 [2, 2048, 11008], P(None, None, 'tp')
- w_down: bfloat16 [2, 11008, 2048], P(None, 'tp')
Outputs:
- output 1: bfloat16 [512, 2048], P('dp'), parts along dimension 0
- output 2: bfloat16 [2, 512, 8, 128], P(None, 'dp', 'tp'), parts along dimension 1
- output 3: bfloat16 [2, 512, 8, 128], P(None, 'dp', 'tp'), parts along dimension 1
There are 2 independent parts. The reference program is written for one: setup_inputs(seed, part) draws one part's arguments, and reference() takes and returns one part's arrays. A program takes and returns all parts, laid end to end along the dimension named above; an argument that names none is the same for every part.
All inputs are finite; a program needn't handle non-finite values.
Results may differ from the reference program's by a relative error of at most 0.0197908.
Values are sent between devices in bfloat16 or wider.
A program may use at most 768 MiB of HBM per device.

```python
import math
import jax
import jax.numpy as jnp
from jax import lax

LAYERS = 2
BATCH_ROWS = 256
CACHE_LEN = 256
D_MODEL = 2048
N_HEADS = 16
KV_HEADS = 2
HEAD_DIM = 128
FF_DIM = 11008
KV_SLOTS = 8

EPS = 1e-6
THETA = 1000000.0


def setup_inputs(seed: int = 0, part: int = 0) -> dict:
    shared_keys = jax.random.split(jax.random.key(seed + 1000), 12)
    own_keys = jax.random.split(jax.random.fold_in(jax.random.key(seed), part), 5)
    repeat_kv = KV_SLOTS // KV_HEADS
    q_width = N_HEADS * HEAD_DIM
    kv_width = KV_SLOTS * HEAD_DIM
    d_scale = D_MODEL ** -0.5

    def normal(key_in, shape_in, scale_val):
        return jax.random.normal(key_in, shape_in, jnp.float32) * scale_val

    def kv_weight(key_in, scale_val):
        base_vals = normal(key_in, (LAYERS, D_MODEL, KV_HEADS, HEAD_DIM), scale_val)
        return jnp.repeat(base_vals, repeat_kv, axis=2).reshape(LAYERS, D_MODEL, kv_width).astype(jnp.bfloat16)

    def kv_bias(key_in, scale_val):
        base_vals = normal(key_in, (LAYERS, KV_HEADS, HEAD_DIM), scale_val)
        return jnp.repeat(base_vals, repeat_kv, axis=1).reshape(LAYERS, kv_width).astype(jnp.bfloat16)

    def draw_cache(key_in, scale_val):
        base_vals = normal(key_in, (LAYERS, BATCH_ROWS, CACHE_LEN, KV_HEADS, HEAD_DIM), scale_val)
        return jnp.repeat(base_vals, repeat_kv, axis=3).astype(jnp.bfloat16)

    lengths = jax.random.randint(own_keys[1], (BATCH_ROWS,), 0, CACHE_LEN, jnp.int32)
    longest = jax.random.randint(own_keys[2], (), 0, BATCH_ROWS, jnp.int32)
    lengths = jnp.where(jnp.arange(BATCH_ROWS) == longest, CACHE_LEN - 1, lengths).astype(jnp.int32)
    return {
        'x_in': normal(own_keys[0], (BATCH_ROWS, D_MODEL), 1.0).astype(jnp.bfloat16),
        'lengths': lengths,
        'k_cache': draw_cache(own_keys[3], 1.5),
        'v_cache': draw_cache(own_keys[4], 1.0),
        'g_attn': (1.0 + normal(shared_keys[0], (LAYERS, D_MODEL), 0.3)).astype(jnp.bfloat16),
        'w_q': normal(shared_keys[1], (LAYERS, D_MODEL, q_width), d_scale).astype(jnp.bfloat16),
        'b_q': normal(shared_keys[2], (LAYERS, q_width), 1.0).astype(jnp.bfloat16),
        'w_k': kv_weight(shared_keys[3], d_scale),
        'b_k': kv_bias(shared_keys[4], 1.5),
        'w_v': kv_weight(shared_keys[5], d_scale),
        'b_v': kv_bias(shared_keys[6], 0.5),
        'w_o': normal(shared_keys[7], (LAYERS, q_width, D_MODEL), q_width ** -0.5).astype(jnp.bfloat16),
        'g_mlp': (1.0 + normal(shared_keys[8], (LAYERS, D_MODEL), 0.3)).astype(jnp.bfloat16),
        'w_gate': normal(shared_keys[9], (LAYERS, D_MODEL, FF_DIM), d_scale).astype(jnp.bfloat16),
        'w_up': normal(shared_keys[10], (LAYERS, D_MODEL, FF_DIM), d_scale).astype(jnp.bfloat16),
        'w_down': normal(shared_keys[11], (LAYERS, FF_DIM, D_MODEL), FF_DIM ** -0.5).astype(jnp.bfloat16),
    }


def rms_scale(x_float, gain_vec):
    mean_sq = jnp.mean(x_float * x_float, axis=-1, keepdims=True)
    return (x_float * lax.rsqrt(mean_sq + EPS) * gain_vec.astype(jnp.float32)).astype(jnp.bfloat16)


def rotary(vec_in, positions):
    half_dim = vec_in.shape[-1] // 2
    inv_freq = jnp.exp(jnp.arange(half_dim, dtype=jnp.float32) * (-2.0 * math.log(THETA) / vec_in.shape[-1]))
    angles = positions.astype(jnp.float32)[:, None, None] * inv_freq
    cos_part = jnp.cos(angles)
    sin_part = jnp.sin(angles)
    lo_half = vec_in[..., :half_dim]
    hi_half = vec_in[..., half_dim:]
    return jnp.concatenate([lo_half * cos_part - hi_half * sin_part, hi_half * cos_part + lo_half * sin_part], axis=-1)


def attend_one(args_in):
    q_rot, key_new, val_new, k_rows, v_rows, length = args_in
    score_scale = q_rot.shape[-1] ** -0.5
    q_float = q_rot.astype(jnp.float32)
    s_old = jnp.einsum('sgh,tsh->sgt', q_float, k_rows.astype(jnp.float32)) * score_scale
    s_new = jnp.einsum('sgh,sh->sg', q_float, key_new.astype(jnp.float32)) * score_scale
    valid_mask = jnp.arange(k_rows.shape[0]) < length
    s_old = jnp.where(valid_mask, s_old, -jnp.inf)
    row_max = jnp.maximum(jnp.max(s_old, axis=-1), s_new)
    w_old = jnp.exp(s_old - row_max[..., None])
    w_new = jnp.exp(s_new - row_max)
    weight_sum = jnp.sum(w_old, axis=-1) + w_new
    mixed_vals = jnp.einsum('sgt,tsh->sgh', w_old.astype(jnp.bfloat16).astype(jnp.float32), v_rows.astype(jnp.float32))
    mixed_vals = mixed_vals + w_new[..., None] * val_new.astype(jnp.float32)[:, None, :]
    return (mixed_vals / weight_sum[..., None]).astype(jnp.bfloat16)


def reference(x_in, lengths, k_cache, v_cache, g_attn, w_q, b_q, w_k, b_k, w_v, b_v, w_o, g_mlp, w_gate, w_up, w_down):
    n_rows = x_in.shape[0]
    head_dim = k_cache.shape[-1]
    n_slots = k_cache.shape[-2]

    def layer_step(x_state, params):
        k_layer, v_layer, g_one, wq_one, bq_one, wk_one, bk_one, wv_one, bv_one, wo_one, g_two, wg_one, wu_one, wd_one = params
        x_float = x_state.astype(jnp.float32)
        hidden = rms_scale(x_float, g_one)
        q_proj = (jnp.dot(hidden, wq_one, preferred_element_type=jnp.float32) + bq_one.astype(jnp.float32)).reshape(n_rows, -1, head_dim)
        k_proj = (jnp.dot(hidden, wk_one, preferred_element_type=jnp.float32) + bk_one.astype(jnp.float32)).reshape(n_rows, n_slots, head_dim)
        v_new = (jnp.dot(hidden, wv_one, preferred_element_type=jnp.float32) + bv_one.astype(jnp.float32)).reshape(n_rows, n_slots, head_dim).astype(jnp.bfloat16)
        q_rot = rotary(q_proj, lengths).astype(jnp.bfloat16).reshape(n_rows, n_slots, -1, head_dim)
        k_new = rotary(k_proj, lengths).astype(jnp.bfloat16)
        attn_rows = lax.map(attend_one, (q_rot, k_new, v_new, k_layer, v_layer, lengths)).reshape(n_rows, -1)
        x_mid = (x_float + jnp.dot(attn_rows, wo_one, preferred_element_type=jnp.float32)).astype(jnp.bfloat16)
        mid_float = x_mid.astype(jnp.float32)
        hidden_two = rms_scale(mid_float, g_two)
        gate_val = jnp.dot(hidden_two, wg_one, preferred_element_type=jnp.float32)
        up_val = jnp.dot(hidden_two, wu_one, preferred_element_type=jnp.float32)
        act_val = (jax.nn.silu(gate_val) * up_val).astype(jnp.bfloat16)
        x_next = (mid_float + jnp.dot(act_val, wd_one, preferred_element_type=jnp.float32)).astype(jnp.bfloat16)
        return x_next, (k_new, v_new)

    x_out, new_rows = lax.scan(layer_step, x_in, (k_cache, v_cache, g_attn, w_q, b_q, w_k, b_k, w_v, b_v, w_o, g_mlp, w_gate, w_up, w_down))
    return x_out, new_rows[0], new_rows[1]
```

```python
import functools
import math
import jax
import jax.numpy as jnp
from jax import lax
from jax.experimental import pallas as pl
from jax.experimental.pallas import tpu as pltpu
from jax.sharding import PartitionSpec as P

EPS = 1e-6
THETA = 1000000.0
MESH = pl.DeviceIdType.MESH
F32 = jnp.float32
BF16 = jnp.bfloat16


def norm_rows(x, gain):
    mean_sq = jnp.mean(x * x, axis=-1, keepdims=True)
    return (x * lax.rsqrt(mean_sq + EPS) * gain).astype(BF16)


def pick(ref, idx):
    both = ref[...].astype(F32)
    return jnp.where(idx == 0, both[0:1], both[1:2])


def dot_nn(a, b):
    return jnp.dot(a, b, preferred_element_type=F32)


def dot_nt(a, b):
    return lax.dot_general(a, b, (((1,), (1,)), ((), ())), preferred_element_type=F32)


def kernel(layers, tp, x_hbm, len_ref, cos_ref, sin_ref, kc_hbm, vc_hbm, ga_ref, wq_hbm, bq_ref, wk_hbm, bk_ref,
           wv_hbm, bv_ref, wo_hbm, gm_ref, wg_hbm, wu_hbm, wd_hbm,
           xo_hbm, kn_hbm, vn_hbm,
           wq_v, wkv_v, wo_v, wg_v, wu_v, wd_v, k_v, v_v,
           part, hbuf, xres, r0, asum, s1, fin,
           qsend, qrecv, kbuf, vbuf, qrows, srows, orows, asend, arecv, act,
           wsem, kvsem, xsem, osem, ssem, rsem, qssem, qrsem):
    i = lax.axis_index("tp")
    chips = tp // 2
    x, c = i // 2, i % 2
    sib = 2 * x + 1 - c
    right = 2 * ((x + 1) % chips) + c
    left = 2 * ((x + chips - 1) % chips) + c
    xr, xl, xo = (x + 1) % chips, (x + chips - 1) % chips, (x + 2) % chips
    idr, idl, ido = 2 * xr + c, 2 * xl + c, 2 * xo + c
    base, m = (i // 4) * 4, i % 4
    cross = base + 3 - m
    width = wg_hbm.shape[1]
    n_seq = k_v.shape[0]

    def load(kind, l):
        copy = pltpu.make_async_copy
        if kind == "q":
            return [copy(wq_hbm.at[l], wq_v, wsem.at[0])]
        if kind == "kv":
            return [copy(wk_hbm.at[l], wkv_v.at[:, 0:128], wsem.at[1]),
                    copy(wv_hbm.at[l], wkv_v.at[:, 128:256], wsem.at[2])]
        if kind == "o":
            return [copy(wo_hbm.at[l], wo_v, wsem.at[3])]
        if kind == "gu":
            return [copy(wg_hbm.at[l], wg_v.at[pl.ds(0, width)], wsem.at[4]),
                    copy(wu_hbm.at[l], wu_v.at[pl.ds(0, width)], wsem.at[5])]
        if kind == "d":
            return [copy(wd_hbm.at[l], wd_v.at[pl.ds(0, width)], wsem.at[6])]
        if kind == "k":
            return [copy(kc_hbm.at[l, pl.ds(m * n_seq, n_seq)], k_v, kvsem.at[0])]
        return [copy(vc_hbm.at[l, pl.ds(m * n_seq, n_seq)], v_v, kvsem.at[1])]

    def start(kind, l):
        for cp in load(kind, l):
            cp.start()

    def wait(kind, l):
        for cp in load(kind, l):
            cp.wait()

    x_copy = pltpu.make_async_copy(x_hbm, part, xsem)
    x_copy.start()
    start("q", 0)
    start("kv", 0)
    start("k", 0)
    start("v", 0)

    barrier = pltpu.get_barrier_semaphore()
    for peer in (sib, right, left, cross):
        pl.semaphore_signal(barrier, inc=1, device_id={"tp": peer}, device_id_type=MESH)

    pad = wg_v.shape[0] - width
    wg_v[pl.ds(width, pad)] = jnp.zeros((pad, wg_v.shape[1]), BF16)
    wu_v[pl.ds(width, pad)] = jnp.zeros((pad, wu_v.shape[1]), BF16)
    wd_v[pl.ds(width, pad)] = jnp.zeros((pad, wd_v.shape[1]), BF16)

    x_copy.wait()
    gain0 = pick(ga_ref, 0)
    for j in range(tp):
        hbuf[j] = norm_rows(part[j // 2, j % 2].astype(F32), gain0)
    xres[...] = part[x, c]
    pl.semaphore_wait(barrier, 4)

    def remote(src, dst, k, dev):
        return pltpu.make_async_remote_copy(src_ref=src, dst_ref=dst, send_sem=ssem.at[k], recv_sem=rsem.at[k],
                                            device_id={"tp": dev}, device_id_type=MESH)

    def reduce_rows():
        order = (xo, xr, xl, x)
        d2d = [remote(part.at[q, 1 - c], r0.at[q], n, sib) for n, q in enumerate(order)]
        for cp in d2d:
            cp.start()
        lo, hi = pl.ds(0, 16), pl.ds(16, 16)

        def chip_sum(n):
            d2d[n].wait_recv()
            return part[order[n], c].astype(F32) + r0[order[n]].astype(F32)

        asum[0] = chip_sum(0).astype(BF16)
        s1r = remote(asum.at[0, lo], s1.at[0], 4, right)
        s1l = remote(asum.at[0, hi], s1.at[1], 5, left)
        s1r.start()
        s1l.start()
        to_right = chip_sum(1)
        asum[1, hi] = to_right[16:32].astype(BF16)
        s2r = remote(asum.at[1, hi], fin.at[0, hi], 6, right)
        s2r.start()
        to_left = chip_sum(2)
        asum[2, lo] = to_left[0:16].astype(BF16)
        s2l = remote(asum.at[2, lo], fin.at[1, lo], 7, left)
        s2l.start()
        s1r.wait_recv()
        asum[1, lo] = (part[xr, c, lo].astype(F32) + r0[xr, lo].astype(F32) + s1[0].astype(F32)).astype(BF16)
        s3r = remote(asum.at[1, lo], fin.at[0, lo], 8, right)
        s3r.start()
        s1l.wait_recv()
        asum[2, hi] = (part[xl, c, hi].astype(F32) + r0[xl, hi].astype(F32) + s1[1].astype(F32)).astype(BF16)
        s3l = remote(asum.at[2, hi], fin.at[1, hi], 9, left)
        s3l.start()
        own = chip_sum(3)
        for cp in (s2r, s2l, s3r, s3l):
            cp.wait_recv()
        total = own + fin[0].astype(F32) + fin[1].astype(F32)
        for cp in d2d + [s1r, s1l, s2r, s2l, s3r, s3l]:
            cp.wait_send()
        return total + xres[...].astype(F32)

    def gather_rows():
        lo, hi = pl.ds(0, 16), pl.ds(16, 16)
        own_r0 = remote(hbuf.at[i, lo], hbuf.at[i, lo], 10, right)
        own_l0 = remote(hbuf.at[i, hi], hbuf.at[i, hi], 11, left)
        own_r1 = remote(hbuf.at[i, hi], hbuf.at[i, hi], 12, right)
        own_l1 = remote(hbuf.at[i, lo], hbuf.at[i, lo], 13, left)
        own_s = remote(hbuf.at[i], hbuf.at[i], 16, sib)
        for cp in (own_r0, own_l0, own_r1, own_l1, own_s):
            cp.start()
        own_r0.wait_recv()
        fwd_r = remote(hbuf.at[idl, lo], hbuf.at[idl, lo], 14, right)
        fwd_r.start()
        own_l0.wait_recv()
        fwd_l = remote(hbuf.at[idr, hi], hbuf.at[idr, hi], 15, left)
        fwd_l.start()
        own_r1.wait_recv()
        sib_l = remote(hbuf.at[idl], hbuf.at[idl], 17, sib)
        sib_l.start()
        own_l1.wait_recv()
        sib_r = remote(hbuf.at[idr], hbuf.at[idr], 18, sib)
        sib_r.start()
        fwd_r.wait_recv()
        sib_o0 = remote(hbuf.at[ido, lo], hbuf.at[ido, lo], 19, sib)
        sib_o0.start()
        fwd_l.wait_recv()
        sib_o1 = remote(hbuf.at[ido, hi], hbuf.at[ido, hi], 20, sib)
        sib_o1.start()
        for cp in (own_s, sib_l, sib_r, sib_o0, sib_o1):
            cp.wait_recv()
        for cp in (own_r0, own_l0, own_r1, own_l1, own_s, fwd_r, fwd_l, sib_l, sib_r, sib_o0, sib_o1):
            cp.wait_send()

    def swap(src, dst, n0):
        copies = []
        for d in (1, 2, 3):
            to = (m + d) % 4
            cp = pltpu.make_async_remote_copy(src_ref=src.at[to], dst_ref=dst.at[m], send_sem=qssem.at[n0 + d - 1],
                                              recv_sem=qrsem.at[n0 + d - 1], device_id={"tp": base + to},
                                              device_id_type=MESH)
            cp.start()
            copies.append(cp)
        dst[m] = src[m]
        return copies

    def turn(v):
        return v * cos_ref[...] + pltpu.roll(v, 64, 1) * sin_ref[...]

    scale = 128.0 ** -0.5

    def layer(l, carry):
        more = l + 1 < layers
        h = hbuf[...].reshape(tp * hbuf.shape[1], hbuf.shape[2])
        wait("q", l)
        wait("kv", l)
        q = dot_nn(h, wq_v[...]) + pick(bq_ref, l)
        for j in range(2):
            qsend[:, :, 128 * j:128 * j + 128] = turn(q[:, 128 * j:128 * j + 128]).astype(BF16).reshape(4, n_seq, 128)
        q_copies = swap(qsend, qrecv, 0)
        kv = dot_nn(h, wkv_v[...])
        kbuf[...] = turn(kv[:, 0:128] + pick(bk_ref, l)).astype(BF16).reshape(4, n_seq, 128)
        vbuf[...] = (kv[:, 128:256] + pick(bv_ref, l)).astype(BF16).reshape(4, n_seq, 128)
        kv_out = [pltpu.make_async_copy(kbuf, kn_hbm.at[l], osem.at[0]),
                  pltpu.make_async_copy(vbuf, vn_hbm.at[l], osem.at[1])]
        for cp in kv_out:
            cp.start()

        @pl.when(more)
        def _():
            start("q", l + 1)
            start("kv", l + 1)

        @pl.when(l == 0)
        def _():
            start("o", l)
            start("gu", l)
            start("d", l)

        for cp in q_copies:
            cp.wait_recv()
        for j in range(8):
            qrows[pl.ds(j, n_seq, stride=8), :] = qrecv[j // 2, :, 128 * (j % 2):128 * (j % 2) + 128].astype(F32)
        wait("k", l)

        def scores(step, carry):
            for u in range(8):
                b = step * 8 + u
                rows = pl.ds(pl.multiple_of(b * 8, 8), 8)
                s = dot_nt(qrows[rows].astype(BF16), k_v[b]) * scale
                t = lax.broadcasted_iota(jnp.int32, s.shape, 1)
                srows[rows] = jnp.where(t < len_ref[m * n_seq + b], s, -jnp.inf)
            return carry

        lax.fori_loop(0, n_seq // 8, scores, 0)
        wait("v", l)

        def mix(step, carry):
            rows = pl.ds(pl.multiple_of(step * 128, 128), 128)
            seqs = pl.ds(pl.multiple_of(step * 16, 16), 16)
            s = srows[rows]
            k16 = jnp.broadcast_to(kbuf[m, seqs].astype(F32)[:, None, :], (16, 8, 128)).reshape(128, 128)
            v16 = jnp.broadcast_to(vbuf[m, seqs].astype(F32)[:, None, :], (16, 8, 128)).reshape(128, 128)
            s_new = jnp.sum(qrows[rows] * k16, axis=-1, keepdims=True) * scale
            top = jnp.maximum(jnp.max(s, axis=-1, keepdims=True), s_new)
            w = jnp.exp(s - top)
            w_new = jnp.exp(s_new - top)
            den = jnp.sum(w, axis=-1, keepdims=True) + w_new
            mixed = jnp.concatenate(
                [dot_nn(w[8 * u:8 * u + 8].astype(BF16), v_v[step * 16 + u]) for u in range(16)], axis=0)
            orows[rows] = (mixed + w_new * v16) / den
            return carry

        lax.fori_loop(0, n_seq // 16, mix, 0)

        @pl.when(more)
        def _():
            start("k", l + 1)
            start("v", l + 1)

        for cp in q_copies:
            cp.wait_send()
        for j in range(8):
            asend[j // 2, :, 128 * (j % 2):128 * (j % 2) + 128] = orows[pl.ds(j, n_seq, stride=8), :].astype(BF16)
        a_copies = swap(asend, arecv, 3)
        wait("o", l)
        for cp in a_copies:
            cp.wait_recv()
        a = arecv[...].reshape(4 * n_seq, 256)
        for j in range(4):
            cols = slice(512 * j, 512 * j + 512)
            part[:, :, :, cols] = dot_nn(a, wo_v[:, cols]).astype(BF16).reshape(part.shape[:3] + (512,))

        @pl.when(more)
        def _():
            start("o", l + 1)

        x_mid = reduce_rows().astype(BF16)
        for cp in a_copies:
            cp.wait_send()
        for cp in kv_out:
            cp.wait()
        xres[...] = x_mid
        hbuf[i] = norm_rows(x_mid.astype(F32), pick(gm_ref, l))
        gather_rows()

        h = hbuf[...].reshape(tp * hbuf.shape[1], hbuf.shape[2])
        wait("gu", l)
        n_act = act.shape[1]
        for lo in range(0, n_act, 256):
            hi = min(lo + 256, n_act)
            gate = dot_nt(h, wg_v[lo:hi])
            up = dot_nt(h, wu_v[lo:hi])
            act[:, lo:hi] = (gate * jax.nn.sigmoid(gate) * up).astype(BF16)

        @pl.when(more)
        def _():
            start("gu", l + 1)

        wait("d", l)
        for j in range(8):
            cols = slice(256 * j, 256 * j + 256)
            part[:, :, :, cols] = dot_nn(act[...], wd_v[:, cols]).astype(BF16).reshape(part.shape[:3] + (256,))

        @pl.when(more)
        def _():
            start("d", l + 1)

        x_next = reduce_rows().astype(BF16)
        xres[...] = x_next
        normed = norm_rows(x_next.astype(F32), pick(ga_ref, jnp.minimum(l + 1, layers - 1)))
        hbuf[i] = jnp.where(more, normed.astype(F32), x_next.astype(F32)).astype(BF16)
        gather_rows()
        return carry

    lax.fori_loop(0, layers, layer, 0)
    out = pltpu.make_async_copy(hbuf, xo_hbm, xsem)
    out.start()
    out.wait()


def solution(mesh):
    cache_spec = P(None, 'dp', None, 'tp', None)
    col_spec = P(None, None, 'tp')
    row_spec = P(None, 'tp', None)
    vec_spec = P(None, 'tp')
    new_spec = P(None, 'dp', 'tp', None)
    in_specs = (P('dp', None), P('dp'), cache_spec, cache_spec, P(), col_spec, vec_spec, col_spec, vec_spec, col_spec, vec_spec, row_spec, P(), col_spec, col_spec, row_spec)
    out_specs = (P('dp', None), new_spec, new_spec)
    tp = mesh.shape['tp']

    def local_step(x_in, lengths, k_cache, v_cache, g_attn, w_q, b_q, w_k, b_k, w_v, b_v, w_o, g_mlp, w_gate, w_up, w_down):
        layers, rows, t_len, _, dim = k_cache.shape
        d_model = x_in.shape[1]
        own, n_seq = rows // tp, rows // 4
        half = dim // 2
        width = w_down.shape[1]
        wide = -(-width // 128) * 128
        inv_freq = jnp.exp(jnp.arange(half, dtype=F32) * (-2.0 * math.log(THETA) / dim))
        angles = lengths.astype(F32)[:, None] * inv_freq
        cos, sin = jnp.cos(angles), jnp.sin(angles)
        cos2 = jnp.concatenate([cos, cos], axis=-1)
        sin2 = jnp.concatenate([-sin, sin], axis=-1)
        any_spec = pl.BlockSpec(memory_space=pl.ANY)
        vmem = pl.BlockSpec(memory_space=pltpu.VMEM)
        smem = pl.BlockSpec(memory_space=pltpu.SMEM)
        x_out, k_new, v_new = pl.pallas_call(
            functools.partial(kernel, layers, tp),
            name="decode",
            out_shape=(jax.ShapeDtypeStruct((tp, own, d_model), BF16),
                       jax.ShapeDtypeStruct((layers, 4, n_seq, dim), BF16),
                       jax.ShapeDtypeStruct((layers, 4, n_seq, dim), BF16)),
            in_specs=[any_spec, smem, vmem, vmem, any_spec, any_spec, vmem, any_spec, vmem, any_spec, vmem,
                      any_spec, vmem, any_spec, vmem, any_spec, any_spec, any_spec],
            out_specs=(any_spec, any_spec, any_spec),
            scratch_shapes=[
                pltpu.VMEM((d_model, 256), BF16),
                pltpu.VMEM((d_model, 256), BF16),
                pltpu.VMEM((256, d_model), BF16),
                pltpu.VMEM((wide, d_model), BF16),
                pltpu.VMEM((wide, d_model), BF16),
                pltpu.VMEM((wide, d_model), BF16),
                pltpu.VMEM((n_seq, t_len, dim), BF16),
                pltpu.VMEM((n_seq, t_len, dim), BF16),
                pltpu.VMEM((tp // 2, 2, own, d_model), BF16),
                pltpu.VMEM((tp, own, d_model), BF16),
                pltpu.VMEM((own, d_model), BF16),
                pltpu.VMEM((tp // 2, own, d_model), BF16),
                pltpu.VMEM((3, own, d_model), BF16),
                pltpu.VMEM((2, own // 2, d_model), BF16),
                pltpu.VMEM((2, own, d_model), BF16),
                pltpu.VMEM((4, n_seq, 256), BF16),
                pltpu.VMEM((4, n_seq, 256), BF16),
                pltpu.VMEM((4, n_seq, dim), BF16),
                pltpu.VMEM((4, n_seq, dim), BF16),
                pltpu.VMEM((n_seq * 8, dim), F32),
                pltpu.VMEM((n_seq * 8, t_len), F32),
                pltpu.VMEM((n_seq * 8, dim), F32),
                pltpu.VMEM((4, n_seq, 256), BF16),
                pltpu.VMEM((4, n_seq, 256), BF16),
                pltpu.VMEM((rows, wide), BF16),
                pltpu.SemaphoreType.DMA((7,)),
                pltpu.SemaphoreType.DMA((2,)),
                pltpu.SemaphoreType.DMA,
                pltpu.SemaphoreType.DMA((2,)),
                pltpu.SemaphoreType.DMA((21,)),
                pltpu.SemaphoreType.DMA((21,)),
                pltpu.SemaphoreType.DMA((6,)),
                pltpu.SemaphoreType.DMA((6,)),
            ],
            compiler_params=pltpu.CompilerParams(collective_id=0, has_side_effects=True, vmem_limit_bytes=60 * 1024 * 1024),
        )(x_in.reshape(tp // 2, 2, own, d_model), lengths, cos2, sin2,
          k_cache.reshape(layers, rows, t_len, dim), v_cache.reshape(layers, rows, t_len, dim),
          g_attn, w_q, b_q, w_k, b_k, w_v, b_v, w_o, g_mlp,
          w_gate.transpose(0, 2, 1), w_up.transpose(0, 2, 1), w_down)
        return (x_out.reshape(rows, d_model), k_new.reshape(layers, rows, 1, dim), v_new.reshape(layers, rows, 1, dim))

    return jax.shard_map(local_step, mesh=mesh, in_specs=in_specs, out_specs=out_specs, check_vma=False)
```
